256 devices in a mesh: row: 16 (over x_lo, y, core), col: 16 (over x_hi, z).
Axes of the slice: x: 4 (x_hi: 2, x_lo: 2; x = x_hi * 2 + x_lo), y: 4, z: 8, core: 2. Of those that a mesh axis runs over, the one named last changes fastest.
Arguments:
- queries: bfloat16 [262144, 768], P(('row', 'col'))
- documents: bfloat16 [8192, 768], P(('row', 'col'))
- counts: int32 [256], P(('row', 'col')), may hold values from 2 to 32, as said below
- positives: int32 [262144], P(('row', 'col')), may hold values from 0 to 8191, as said below
Outputs:
- losses: float32 [262144], P(('row', 'col'))
The draws below stay inside these ranges and needn't reach their ends.
Inputs may be any that keep to these rules, and one draw needn't show every extreme that they name: `counts`: some block has exactly 32 valid slots in every draw. Each names a valid slot: positives[i] % 32 < counts[positives[i] // 32].
All inputs are finite; a program needn't handle non-finite values.
Results may differ from the reference program's by a relative error of at most 0.0003.
Values may be sent and summed in bfloat16 or wider, within the bound.
No kernel may reach another device: no remote copies, remote signals or barrier semaphores. Data moves between devices by JAX's collectives and lax.ppermute only.
A program may use at most 128 MiB of HBM per device.

```python
import jax
import jax.numpy as jnp
from jax import lax

D = 768
Q_DEV = 1024
DOC_DEV = 32
QUERIES = 262144
DOCS = 8192
DEVICES = 256


def shared_ints(key):
    counts = jax.random.randint(jax.random.fold_in(key, 11), (DEVICES,), 2, DOC_DEV + 1)
    full = jax.random.randint(jax.random.fold_in(key, 13), (), 0, DEVICES)
    counts = jnp.where(jnp.arange(DEVICES) == full, DOC_DEV, counts).astype(jnp.int32)
    owner = jax.random.randint(jax.random.fold_in(key, 12), (QUERIES,), 0, DEVICES)
    raw = jax.random.randint(jax.random.fold_in(key, 14), (QUERIES,), 0, 1000000)
    slot = raw % counts[owner]
    return (counts, (owner * DOC_DEV + slot).astype(jnp.int32))


def shared_floats(key):
    docs = jax.random.normal(jax.random.fold_in(key, 21), (DOCS, D), jnp.float32)
    quer = jax.random.normal(jax.random.fold_in(key, 22), (QUERIES, D), jnp.float32)
    return (quer, docs)


def draw_queries(key, part):
    return shared_floats(key)[0].astype(jnp.bfloat16)


def draw_documents(key, part):
    return shared_floats(key)[1].astype(jnp.bfloat16)


def draw_counts(key, part):
    return shared_ints(key)[0]


def draw_positives(key, part):
    return shared_ints(key)[1]


def setup_inputs(seed: int = 0) -> dict:
    splits = jax.random.split(jax.random.key(seed), 5)
    return {
        "queries": draw_queries(jax.random.fold_in(splits[4], 71), 0),
        "documents": draw_documents(jax.random.fold_in(splits[4], 71), 0),
        "counts": draw_counts(jax.random.fold_in(splits[4], 71), 0),
        "positives": draw_positives(jax.random.fold_in(splits[4], 71), 0),
    }


def reference(queries, documents, counts, positives):
    slot = jnp.arange(DOCS, dtype=jnp.int32)
    valid = (slot % DOC_DEV) < counts[slot // DOC_DEV]
    total = jnp.sum(counts.astype(jnp.float32))
    scale = D ** -0.5
    query_blocks = queries.reshape(DEVICES, Q_DEV, D)
    pos_blocks = positives.reshape(DEVICES, Q_DEV)

    def one_block(pair):
        block, wanted = pair
        scores = jnp.dot(block, documents.T, preferred_element_type=jnp.float32) * scale
        masked = jnp.where(valid[None, :], scores, -1e30)
        top = jnp.max(masked, axis=1)
        lse = top + jnp.log(jnp.sum(jnp.exp(masked - top[:, None]), axis=1))
        picked = jnp.take_along_axis(scores, wanted[:, None].astype(jnp.int32), axis=1)[:, 0]
        return lse - picked - jnp.log(total)

    return lax.map(one_block, (query_blocks, pos_blocks)).reshape(QUERIES)
```

```python
import functools

import jax
import jax.numpy as jnp
import numpy as np
from jax import lax
from jax.experimental import pallas as pl
from jax.experimental.pallas import tpu as pltpu
from jax.sharding import Mesh
from jax.sharding import PartitionSpec as P

AXES = ("x_lo", "y", "core", "x_hi", "z")
TORUS = (4, 4, 8)
CORES = 2
LOW = -1e30
LOG2E = 1.4426950408889634
TILE_D = 512
TILE_Q = 512
ROUNDS = (
    ((0, 0, 4),),
    ((1, -1, 1), (-1, 1, -1), (2, 2, 2)),
    ((1, 1, 0), (-1, -1, 0), (0, 0, 2)),
    ((1, 0, 0), (0, 1, 0), (0, 0, 1)),
)
LAST_SPLIT = 2


def flat(x, y, z, c):
    return (((x % 2 * 4 + y) * 2 + c) * 2 + x // 2) * 8 + z


def everyone():
    return [(x, y, z, c) for x in range(4) for y in range(4) for z in range(8) for c in range(2)]


def wrap(chip):
    return tuple(int(v) % n for v, n in zip(chip, TORUS))


def by_offset(value, offset):
    pairs = []
    for x, y, z, c in everyone():
        sign = 1 if c == 0 else -1
        to = wrap((x + sign * offset[0], y + sign * offset[1], z + sign * offset[2]))
        pairs.append((flat(x, y, z, c), flat(*to, c)))
    return lax.ppermute(value, AXES, pairs)


def to_partner(value):
    return lax.ppermute(value, "core", [(0, 1), (1, 0)])


def gather(block):
    held, buffer = [(0, 0, 0)], block
    moved = lambda blocks, offset: [wrap(np.subtract(a, offset)) for a in blocks]
    for offsets in ROUNDS[:-1]:
        parts = [by_offset(buffer, o) for o in offsets]
        held = held + [a for o in offsets for a in moved(held, o)]
        buffer = jnp.concatenate([buffer] + parts, axis=0)
    groups, order = [[buffer]], list(held)
    rows, count = buffer.shape[0] // LAST_SPLIT, len(held) // LAST_SPLIT
    for s in range(LAST_SPLIT):
        groups.append([by_offset(buffer[s * rows : (s + 1) * rows], o) for o in ROUNDS[-1]])
        for o in ROUNDS[-1]:
            order += moved(held[s * count : (s + 1) * count], o)
    return groups, order


def first_indices(order, slots):
    x = lax.axis_index("x_hi") * 2 + lax.axis_index("x_lo")
    y, z, c = lax.axis_index("y"), lax.axis_index("z"), lax.axis_index("core")
    sign = 1 - 2 * c
    table = np.asarray(order, np.int32)
    bx = (x + sign * table[:, 0]) % TORUS[0]
    by = (y + sign * table[:, 1]) % TORUS[1]
    bz = (z + sign * table[:, 2]) % TORUS[2]
    return (flat(bx, by, bz, c) * slots).astype(jnp.int32)


def kernel(first, last, block0, slots, scale, n_docs, *refs):
    firsts = refs[0]
    docs = refs[1 : 1 + n_docs]
    queries, wanted = refs[1 + n_docs : 3 + n_docs]
    rest = refs[3 + n_docs :]
    if not first:
        top_in, sum_in, hit_in, count_in = rest[:4]
        rest = rest[4:]
    if last:
        mine, theirs, top, total, hit, count, scores = rest
    else:
        top, total, hit, count, scores = rest
    width = queries.shape[1]
    if first:
        top[...] = jnp.full(top.shape, LOW, jnp.float32)
        total[...] = jnp.zeros(total.shape, jnp.float32)
        hit[...] = jnp.zeros(hit.shape, jnp.float32)
        count[...] = jnp.zeros(count.shape, jnp.float32)
    else:
        top[...] = top_in[...]
        total[...] = sum_in[...]
        hit[...] = hit_in[...]
        count[...] = count_in[...]
    tiles = []
    block = block0
    for ref in docs:
        for row in range(0, ref.shape[0], TILE_D):
            tiles.append((ref, row, block))
            block += TILE_D // slots
    n = len(tiles)
    steps = width // TILE_Q
    factor = scale * LOG2E
    lanes = TILE_Q // 128
    iota = lax.broadcasted_iota(jnp.int32, (8, 128), 0)

    def multiply(j, q):
        ref, row, _ = tiles[j]
        at = pl.multiple_of(q * TILE_Q, TILE_Q)
        scores[j] = jnp.dot(
            ref[row : row + TILE_D, :], queries[:, pl.ds(at, TILE_Q)], preferred_element_type=jnp.float32
        )

    def consume(j, q):
        ref, row, block = tiles[j]
        at = [pl.ds(pl.multiple_of(q * TILE_Q + 128 * l, 128), 128) for l in range(lanes)]
        want = [jnp.broadcast_to(wanted[:, a], (8, 128)) for a in at]
        old = [top[:, a] for a in at]
        new = list(old)
        found = [hit[:, a] for a in at]
        seen = count[...]
        for r in range(0, TILE_D, 16):
            marks = ref[row + r : row + r + 16, 0:128].astype(jnp.float32)
            base = firsts[block + r // slots]
            for h in range(2):
                mark = marks[8 * h : 8 * h + 8]
                valid = mark == mark
                seen = seen + jnp.where(valid, 1.0, 0.0)
                index = iota + (base + (r + 8 * h) % slots)
                for l in range(lanes):
                    part = (j, pl.ds(r + 8 * h, 8), pl.ds(128 * l, 128))
                    s = jnp.where(valid, scores[part], LOW)
                    scores[part] = s
                    new[l] = jnp.maximum(new[l], s)
                    found[l] = jnp.where(index == want[l], s, found[l])
        acc = [total[:, a] * jnp.exp2((o - m) * factor) for a, o, m in zip(at, old, new)]
        for r in range(0, TILE_D, 8):
            for l in range(lanes):
                s = scores[j, pl.ds(r, 8), pl.ds(128 * l, 128)]
                acc[l] = acc[l] + jnp.exp2((s - new[l]) * factor)
        for l in range(lanes):
            top[:, at[l]] = new[l]
            total[:, at[l]] = acc[l]
            hit[:, at[l]] = found[l]
        count[...] = seen

    multiply(0, 0)

    def step(q, carry):
        for j in range(n):
            if j + 1 < n:
                multiply(j + 1, q)
            else:
                multiply(0, jnp.minimum(q + 1, steps - 1))
            consume(j, q)
        return carry

    lax.fori_loop(0, steps, step, 0)
    if last:
        m = jnp.max(top[...], axis=0, keepdims=True)
        s = jnp.sum(total[...] * jnp.exp2((top[...] - m) * factor), axis=0, keepdims=True)
        p = jnp.sum(hit[...], axis=0, keepdims=True)
        seen = jnp.sum(count[...], axis=0, keepdims=True) * (1.0 / steps)
        half = width // 2
        seen = jnp.concatenate([seen] * (half // 128), axis=1)
        for out, a in ((mine, 0), (theirs, half)):
            out[0:1, :] = m[:, a : a + half]
            out[1:2, :] = s[:, a : a + half]
            out[2:3, :] = p[:, a : a + half]
            out[3:4, :] = seen


def chunk(docs, firsts, queries, wanted, carry, last, block0, slots, scale):
    width = queries.shape[1]
    state = [jax.ShapeDtypeStruct((8, width), jnp.float32)] * 3 + [jax.ShapeDtypeStruct((8, 128), jnp.float32)]
    vmem = pl.BlockSpec(memory_space=pltpu.VMEM)
    n = sum(d.shape[0] for d in docs)
    scratch = [pltpu.VMEM((n // TILE_D, TILE_D, TILE_Q), jnp.float32)]
    if last:
        out = [jax.ShapeDtypeStruct((4, width // 2), jnp.float32)] * 2
        scratch = [pltpu.VMEM(s.shape, s.dtype) for s in state] + scratch
    else:
        out = state
    given = [*docs, queries, wanted, *(carry or ())]
    return pl.pallas_call(
        functools.partial(kernel, carry is None, last, block0, slots, scale, len(docs)),
        out_shape=out,
        in_specs=[pl.BlockSpec(memory_space=pltpu.SMEM)] + [vmem] * len(given),
        out_specs=[vmem] * len(out),
        scratch_shapes=scratch,
        cost_estimate=pl.CostEstimate(
            flops=2 * n * width * queries.shape[0], bytes_accessed=2 * n * queries.shape[0], transcendentals=n * width
        ),
        compiler_params=pltpu.CompilerParams(vmem_limit_bytes=24 * 1024 * 1024),
    )(firsts, *given)


def shards(queries, documents, counts, positives):
    slots, feat = documents.shape
    scale = feat ** (-0.5)
    slot = lax.broadcasted_iota(jnp.int32, documents.shape, 0)
    marked = jnp.where(slot < counts[0], documents, jnp.bfloat16(jnp.nan))
    groups, order = gather(marked)
    both = jnp.concatenate([queries, to_partner(queries)], axis=0).T
    wanted = positives[None, :]
    wanted = jnp.concatenate([wanted, to_partner(wanted)], axis=1)
    firsts = first_indices(order, slots)
    carry, block = None, 0
    for k, docs in enumerate(groups):
        carry = chunk(docs, firsts, both, wanted, carry, k == len(groups) - 1, block, slots, scale)
        block += sum(d.shape[0] for d in docs) // slots
    mine, theirs = carry
    other = to_partner(theirs)
    top = jnp.maximum(mine[0], other[0])
    total = mine[1] * jnp.exp((mine[0] - top) * scale) + other[1] * jnp.exp((other[0] - top) * scale)
    lse = top * scale + jnp.log(total)
    return lse - (mine[2] + other[2]) * scale - jnp.log(mine[3] + other[3])


def solution(mesh):
    finer = Mesh(mesh.devices.reshape(2, 4, 2, 2, 8), AXES)
    return jax.shard_map(
        shards,
        mesh=finer,
        in_specs=(P(AXES, None), P(AXES, None), P(AXES), P(AXES)),
        out_specs=P(AXES),
        check_vma=False,
    )
```

```python
import functools

import jax
import jax.numpy as jnp
import numpy as np
from jax import lax
from jax.experimental import pallas as pl
from jax.experimental.pallas import tpu as pltpu
from jax.sharding import Mesh
from jax.sharding import PartitionSpec as P


AXES = ("x_lo", "y", "core", "x_hi", "z")
TORUS = (4, 4, 8)
LOW = -1e30
LOG2E = 1.4426950408889634
TILE_Q = 512
LANES = 128
EXTRA = 16
PIECES = 1
AHEAD = 3
UNROLL = 2
VMEM_LIMIT = 60 * 1024 * 1024
NEAR = (((0, 0, 4),), ((2, 2, 2), (-1, 1, -1), (1, -1, 1)))
FAR = ((1, 1, 0), (-1, -1, 0), (0, 0, 2))
NEIGHBOURS = ((1, 0, 0), (0, 1, 0), (0, 0, 1))


def flat(x, y, z, c):
    return (((x % 2 * 4 + y) * 2 + c) * 2 + x // 2) * 8 + z


def wrap(chip):
    return tuple(int(v) % n for v, n in zip(chip, TORUS))


def by_offset(value, offset):
    pairs = []
    for x in range(4):
        for y in range(4):
            for z in range(8):
                for c in range(2):
                    sign = 1 - 2 * c
                    to = wrap((x + sign * offset[0], y + sign * offset[1], z + sign * offset[2]))
                    pairs.append((flat(x, y, z, c), flat(*to, c)))
    return lax.ppermute(value, AXES, pairs)


def to_partner(value):
    return lax.ppermute(value, "core", [(0, 1), (1, 0)])


def moved(blocks, offset):
    return [wrap(np.subtract(a, offset)) for a in blocks]


def first_indices(parts, slots):
    x = lax.axis_index("x_hi") * 2 + lax.axis_index("x_lo")
    y, z, c = lax.axis_index("y"), lax.axis_index("z"), lax.axis_index("core")
    table = np.concatenate([np.asarray(p + p, np.int32) for p in parts])
    other = np.concatenate([np.repeat(np.int32([0, 1]), len(p)) for p in parts])
    core = (c + other) % 2
    sign = 1 - 2 * core
    bx = (x + sign * table[:, 0]) % TORUS[0]
    by = (y + sign * table[:, 1]) % TORUS[1]
    bz = (z + sign * table[:, 2]) % TORUS[2]
    return (flat(bx, by, bz, core) * slots).astype(jnp.int32)


def prepare(queries_ref, wanted_ref, *out_refs):
    rows, feat = queries_ref.shape
    wanted = wanted_ref[...]
    high = (wanted // LANES).astype(jnp.float32)
    low = (wanted % LANES).astype(jnp.float32)
    row = lax.broadcasted_iota(jnp.int32, (EXTRA, rows), 0)
    codes = jnp.where(row == 0, high, jnp.where(row == 1, low, 0.0)).astype(queries_ref.dtype)
    for k, out in enumerate(out_refs):
        at = slice(k * TILE_Q, (k + 1) * TILE_Q)
        out[0:feat, :] = queries_ref[at, :].T
        out[feat : feat + EXTRA, :] = codes[:, at]


def prepared(queries, positives):
    rows, feat = queries.shape
    vmem = pl.BlockSpec(memory_space=pltpu.VMEM)
    tiles = rows // TILE_Q
    return pl.pallas_call(
        prepare,
        out_shape=[jax.ShapeDtypeStruct((feat + EXTRA, TILE_Q), queries.dtype)] * tiles,
        in_specs=[vmem] * 2,
        out_specs=[vmem] * tiles,
        cost_estimate=pl.CostEstimate(flops=2**26, bytes_accessed=4 * rows * feat, transcendentals=0),
        compiler_params=pltpu.CompilerParams(vmem_limit_bytes=16 * 1024 * 1024),
    )(queries, positives[None, :])


def kernel(first, last, block0, slots, scale, n_docs, n_asked, per, n_tiles, *refs):
    firsts = refs[0]
    doc_parts = refs[1 : 1 + n_docs]
    asked = refs[1 + n_docs : 1 + n_docs + n_asked]
    rest = refs[1 + n_docs + n_asked :]
    if not first:
        given, rest = rest[:4], rest[4:]
    if last:
        results, rest = rest[: n_asked // per], rest[n_asked // per :]
    top, total, hit, count, docs, tiles, scores, doc_here, tile_here = rest
    part_rows, feat = doc_parts[0].shape
    rows = docs.shape[1]
    factor = scale * LOG2E
    lanes = TILE_Q // LANES
    iota = lax.broadcasted_iota(jnp.int32, (8, LANES), 0)
    inside = rows // part_rows
    doc_copies = [
        pltpu.make_async_copy(p, docs.at[k // inside, pl.ds(k % inside * part_rows, part_rows)], doc_here.at[k])
        for k, p in enumerate(doc_parts)
    ]

    def fetch(i):
        deep = asked[i].shape[0] // PIECES
        for p in range(PIECES):
            at = pl.ds(p * deep, deep)
            pltpu.make_async_copy(asked[i].at[at], tiles.at[i, at], tile_here.at[i]).start()

    for copy in doc_copies[:inside]:
        copy.start()
    fetch(0)
    for copy in doc_copies[inside:]:
        copy.start()
    for i in range(1, AHEAD):
        fetch(i)

    def arrive(i):
        pltpu.make_async_copy(asked[0], tiles.at[i], tile_here.at[i]).wait()

    def multiply(t, i):
        scores[t % 2] = jnp.dot(docs[t % n_tiles], tiles[i, 0:feat, :], preferred_element_type=jnp.float32)

    def consume(t, i):
        j, where = t % n_tiles, t % 2
        at = [pl.ds(pl.multiple_of(i * TILE_Q + LANES * l, LANES), LANES) for l in range(lanes)]
        codes = tiles[i, feat : feat + EXTRA, :].astype(jnp.float32)
        codes = (codes[0:1, :] * LANES + codes[1:2, :]).astype(jnp.int32)
        want = [jnp.broadcast_to(codes[:, LANES * l : LANES * (l + 1)], (8, LANES)) for l in range(lanes)]
        old = [top[:, a] for a in at]
        new = list(old)
        found = [hit[:, a] for a in at]
        seen = count[...]
        for r in range(0, rows, 16):
            marks = docs[j, r : r + 16, 0:LANES].astype(jnp.float32)
            base = firsts[block0 + (j * rows + r) // slots]
            for h8 in (0, 8):
                mark = marks[h8 : h8 + 8]
                valid = mark == mark
                seen = seen + jnp.where(valid, 1.0, 0.0)
                index = iota + (base + (r + h8) % slots)
                for l in range(lanes):
                    part = (where, pl.ds(r + h8, 8), pl.ds(LANES * l, LANES))
                    s = jnp.where(valid, scores[part], LOW)
                    scores[part] = s
                    new[l] = jnp.maximum(new[l], s)
                    found[l] = jnp.where(index == want[l], s, found[l])
        acc = [total[:, a] * jnp.exp2((o - m) * factor) for a, o, m in zip(at, old, new)]
        for r in range(0, rows, 8):
            for l in range(lanes):
                s = scores[where, pl.ds(r, 8), pl.ds(LANES * l, LANES)]
                acc[l] = acc[l] + jnp.exp2((s - new[l]) * factor)
        for l in range(lanes):
            top[:, at[l]] = new[l]
            total[:, at[l]] = acc[l]
            hit[:, at[l]] = found[l]
        count[...] = seen

    if first:
        top[...] = jnp.full(top.shape, LOW, jnp.float32)
        for ref in (total, hit, count):
            ref[...] = jnp.zeros(ref.shape, jnp.float32)
    else:
        for ref, old in zip((top, total, hit, count), given):
            ref[...] = old[...]
    for copy in doc_copies[:inside]:
        copy.wait()
    arrive(0)
    multiply(0, 0)
    for copy in doc_copies[inside:]:
        copy.wait()

    def step(g, carry):
        n = UNROLL * n_tiles
        for t in range(n):
            i = g * UNROLL + t // n_tiles
            if t % n_tiles == 0:
                for k in range(AHEAD, n_asked):
                    pl.when(i + AHEAD == k)(functools.partial(fetch, k))
            if (t + 1) % n_tiles == 0:
                pl.when(i + 1 < n_asked)(functools.partial(arrive, jnp.minimum(i + 1, n_asked - 1)))
            multiply((t + 1) % n, jnp.minimum(g * UNROLL + (t + 1) // n_tiles, n_asked - 1))
            consume(t, i)
        return carry

    lax.fori_loop(0, n_asked // UNROLL, step, 0)
    if last:
        width = per * TILE_Q
        m = jnp.max(top[...], axis=0, keepdims=True)
        s = jnp.sum(total[...] * jnp.exp2((top[...] - m) * factor), axis=0, keepdims=True)
        p = jnp.sum(hit[...], axis=0, keepdims=True)
        seen = jnp.sum(count[...], axis=0, keepdims=True) * (1.0 / n_asked)
        seen = jnp.concatenate([seen] * (width // LANES), axis=1)
        for b, out in enumerate(results):
            at = slice(b * width, (b + 1) * width)
            out[0:1, :] = m[:, at]
            out[1:2, :] = s[:, at]
            out[2:3, :] = p[:, at]
            out[3:4, :] = seen


def chunk(docs, tile_rows, firsts, asked, per, carry, last, block0, slots, scale):
    deep = asked[0].shape[0]
    rows, feat = docs[0].shape
    width = len(asked) * TILE_Q
    n_tiles = len(docs) * rows // tile_rows
    state = [((8, width), jnp.float32)] * 3 + [((8, LANES), jnp.float32)]
    vmem, hbm = pl.BlockSpec(memory_space=pltpu.VMEM), pl.BlockSpec(memory_space=pltpu.HBM)
    scratch = [
        pltpu.VMEM((n_tiles, tile_rows, feat), jnp.bfloat16),
        pltpu.VMEM((len(asked), deep, TILE_Q), jnp.bfloat16),
        pltpu.VMEM((2, tile_rows, TILE_Q), jnp.float32),
        pltpu.SemaphoreType.DMA((len(docs),)),
        pltpu.SemaphoreType.DMA((len(asked),)),
    ]
    if last:
        out = [jax.ShapeDtypeStruct((4, per * TILE_Q), jnp.float32)] * (len(asked) // per)
        scratch = [pltpu.VMEM(*s) for s in state] + scratch
    else:
        out = [jax.ShapeDtypeStruct(*s) for s in state]
    work = len(docs) * rows * width
    return pl.pallas_call(
        functools.partial(kernel, carry is None, last, block0, slots, scale, len(docs), len(asked), per, n_tiles),
        out_shape=out,
        in_specs=[pl.BlockSpec(memory_space=pltpu.SMEM)]
        + [hbm] * (len(docs) + len(asked))
        + [vmem] * len(carry or ()),
        out_specs=[vmem] * len(out),
        scratch_shapes=scratch,
        cost_estimate=pl.CostEstimate(flops=2 * work * feat, bytes_accessed=2 * deep * width, transcendentals=work),
        compiler_params=pltpu.CompilerParams(vmem_limit_bytes=VMEM_LIMIT),
    )(firsts, *docs, *asked, *(carry or ()))


def losses_of(queries, documents, counts, positives):
    slots, feat = documents.shape
    scale = feat ** (-0.5)
    slot = lax.broadcasted_iota(jnp.int32, documents.shape, 0)
    buffer = jnp.where(slot < counts[0], documents, jnp.bfloat16(jnp.nan))
    asked = list(prepared(queries, positives))
    per = len(asked)
    for o in NEIGHBOURS:
        asked += [by_offset(asked[h], o) for h in range(per)]
    held = [(0, 0, 0)]
    for offsets in NEAR:
        pieces = [by_offset(buffer, o) for o in offsets]
        held = held + [a for o in offsets for a in moved(held, o)]
        buffer = jnp.concatenate([buffer] + pieces, axis=0)
    parts = [buffer] + [by_offset(buffer, o) for o in FAR]
    firsts = first_indices([held, sum([moved(held, o) for o in FAR], [])], slots)
    theirs = [to_partner(part) for part in parts]
    common = (firsts, asked, per)
    rows = buffer.shape[0]
    carry = chunk([parts[0], theirs[0]], rows, *common, None, False, 0, slots, scale)
    carry = chunk(parts[1:] + theirs[1:], 2 * rows, *common, carry, True, 2 * len(held), slots, scale)
    answers = [carry[0]] + [by_offset(a, [-v for v in o]) for a, o in zip(carry[1:], NEIGHBOURS)]
    top = functools.reduce(jnp.maximum, [a[0] for a in answers])
    total = sum(a[1] * jnp.exp((a[0] - top) * scale) for a in answers)
    hit = sum(a[2] for a in answers)
    seen = sum(a[3] for a in answers)
    return top * scale + jnp.log(total) - hit * scale - jnp.log(seen)


def solution(mesh):
    finer = Mesh(mesh.devices.reshape(2, 4, 2, 2, 8), AXES)
    return jax.shard_map(
        losses_of,
        mesh=finer,
        in_specs=(P(AXES, None), P(AXES, None), P(AXES), P(AXES)),
        out_specs=P(AXES),
        check_vma=False,
    )
```

```python
import functools

import jax
import jax.numpy as jnp
import numpy as np
from jax import lax
from jax.experimental import pallas as pl
from jax.experimental.pallas import tpu as pltpu
from jax.sharding import Mesh
from jax.sharding import PartitionSpec as P


AXES = ("x_lo", "y", "core", "x_hi", "z")
TORUS = (4, 4, 8)
LOW = -1e30
LOG2E = 1.4426950408889634
TILE_Q = 512
LANES = 128
EXTRA = 16
AHEAD = 2
VMEM_LIMIT = 16 * 1024 * 1024
NEAR = (((0, 0, 4),), ((2, 2, 2), (-1, 1, -1), (1, -1, 1)))
FAR = ((1, 1, 0), (-1, -1, 0), (0, 0, 2))
NEIGHBOURS = ((1, 0, 0), (0, 1, 0), (0, 0, 1))


def flat(x, y, z, c):
    return (((x % 2 * 4 + y) * 2 + c) * 2 + x // 2) * 8 + z


def wrap(chip):
    return tuple(int(v) % n for v, n in zip(chip, TORUS))


def by_offset(value, offset):
    pairs = []
    for x in range(4):
        for y in range(4):
            for z in range(8):
                for c in range(2):
                    sign = 1 - 2 * c
                    to = wrap((x + sign * offset[0], y + sign * offset[1], z + sign * offset[2]))
                    pairs.append((flat(x, y, z, c), flat(*to, c)))
    return lax.ppermute(value, AXES, pairs)


def to_partner(value):
    return lax.ppermute(value, "core", [(0, 1), (1, 0)])


def moved(blocks, offset):
    return [wrap(np.subtract(a, offset)) for a in blocks]


def first_indices(parts, slots):
    x = lax.axis_index("x_hi") * 2 + lax.axis_index("x_lo")
    y, z, c = lax.axis_index("y"), lax.axis_index("z"), lax.axis_index("core")
    table = np.concatenate([np.asarray(p + p, np.int32) for p in parts])
    other = np.concatenate([np.repeat(np.int32([0, 1]), len(p)) for p in parts])
    core = (c + other) % 2
    sign = 1 - 2 * core
    bx = (x + sign * table[:, 0]) % TORUS[0]
    by = (y + sign * table[:, 1]) % TORUS[1]
    bz = (z + sign * table[:, 2]) % TORUS[2]
    return (flat(bx, by, bz, core) * slots).astype(jnp.int32)


def prepare(queries_ref, wanted_ref, *out_refs):
    rows, feat = queries_ref.shape
    wanted = wanted_ref[...]
    high = (wanted // LANES).astype(jnp.float32)
    low = (wanted % LANES).astype(jnp.float32)
    row = lax.broadcasted_iota(jnp.int32, (EXTRA, rows), 0)
    codes = jnp.where(row == 0, high, jnp.where(row == 1, low, 0.0)).astype(queries_ref.dtype)
    for k, out in enumerate(out_refs):
        at = slice(k * TILE_Q, (k + 1) * TILE_Q)
        out[0:feat, :] = queries_ref[at, :].T
        out[feat : feat + EXTRA, :] = codes[:, at]


def prepared(queries, positives):
    rows, feat = queries.shape
    vmem = pl.BlockSpec(memory_space=pltpu.VMEM)
    tiles = rows // TILE_Q
    return pl.pallas_call(
        prepare,
        out_shape=[jax.ShapeDtypeStruct((feat + EXTRA, TILE_Q), queries.dtype)] * tiles,
        in_specs=[vmem] * 2,
        out_specs=[vmem] * tiles,
        cost_estimate=pl.CostEstimate(flops=2**26, bytes_accessed=4 * rows * feat, transcendentals=0),
        compiler_params=pltpu.CompilerParams(vmem_limit_bytes=16 * 1024 * 1024),
    )(queries, positives[None, :])


def kernel(plan, block0, slots, scale, *refs):
    n_docs, n_asked, loops, carried, results = plan
    firsts = refs[0]
    doc_parts = refs[1 : 1 + n_docs]
    asked = refs[1 + n_docs : 1 + n_docs + n_asked]
    rest = refs[1 + n_docs + n_asked :]
    if carried:
        given, rest = rest[:4], rest[4:]
    if results:
        answers, rest = rest[: len(results)], rest[len(results) :]
    top, total, hit, count, docs, tiles, scores, doc_here, tile_here = rest
    part_rows, feat = doc_parts[0].shape
    rows = docs.shape[1]
    factor = scale * LOG2E
    lanes = TILE_Q // LANES
    iota = lax.broadcasted_iota(jnp.int32, (8, LANES), 0)
    inside = rows // part_rows
    doc_copies = [
        pltpu.make_async_copy(p, docs.at[k // inside, pl.ds(k % inside * part_rows, part_rows)], doc_here.at[k])
        for k, p in enumerate(doc_parts)
    ]
    tile_copies = [pltpu.make_async_copy(q, tiles.at[i], tile_here.at[i]) for i, q in enumerate(asked)]
    ahead = min(AHEAD, n_asked)
    for copy in doc_copies[:inside] + tile_copies[:1] + doc_copies[inside:] + tile_copies[1:ahead]:
        copy.start()

    def arrive(i):
        pltpu.make_async_copy(asked[0], tiles.at[i], tile_here.at[i]).wait()

    def multiply(j, where, i):
        scores[where] = jnp.dot(docs[j], tiles[i, 0:feat, :], preferred_element_type=jnp.float32)

    def consume(j, where, i):
        at = [pl.ds(pl.multiple_of(i * TILE_Q + LANES * l, LANES), LANES) for l in range(lanes)]
        codes = tiles[i, feat : feat + EXTRA, :].astype(jnp.float32)
        codes = (codes[0:1, :] * LANES + codes[1:2, :]).astype(jnp.int32)
        want = [jnp.broadcast_to(codes[:, LANES * l : LANES * (l + 1)], (8, LANES)) for l in range(lanes)]
        old = [top[:, a] for a in at]
        new = list(old)
        found = [hit[:, a] for a in at]
        seen = count[...]
        for r in range(0, rows, 16):
            marks = docs[j, r : r + 16, 0:LANES].astype(jnp.float32)
            base = firsts[block0 + (j * rows + r) // slots]
            for h8 in (0, 8):
                mark = marks[h8 : h8 + 8]
                valid = mark == mark
                seen = seen + jnp.where(valid, 1.0, 0.0)
                index = iota + (base + (r + h8) % slots)
                for l in range(lanes):
                    part = (where, pl.ds(r + h8, 8), pl.ds(LANES * l, LANES))
                    s = jnp.where(valid, scores[part], LOW)
                    scores[part] = s
                    new[l] = jnp.maximum(new[l], s)
                    found[l] = jnp.where(index == want[l], s, found[l])
        acc = [total[:, a] * jnp.exp2((o - m) * factor) for a, o, m in zip(at, old, new)]
        for r in range(0, rows, 8):
            for l in range(lanes):
                s = scores[where, pl.ds(r, 8), pl.ds(LANES * l, LANES)]
                acc[l] = acc[l] + jnp.exp2((s - new[l]) * factor)
        for l in range(lanes):
            top[:, at[l]] = new[l]
            total[:, at[l]] = acc[l]
            hit[:, at[l]] = found[l]
        count[...] = seen

    count[...] = jnp.zeros(count.shape, jnp.float32)
    top[...] = jnp.full(top.shape, LOW, jnp.float32)
    total[...] = jnp.zeros(total.shape, jnp.float32)
    hit[...] = jnp.zeros(hit.shape, jnp.float32)
    for copy in doc_copies[:inside]:
        copy.wait()
    arrive(0)
    multiply(loops[0][2][0], 0, 0)
    if carried:
        skip, kept, _ = carried
        for ref, old in zip((top, total, hit), given):
            ref[:, 0 : kept * TILE_Q] = old[:, skip * TILE_Q : (skip + kept) * TILE_Q]
    for copy in doc_copies[inside:]:
        copy.wait()
    for begin, end, order in loops:
        n = len(order)
        turns = 2 if n % 2 == 0 else n

        def step(i, carry):
            later = jnp.minimum(i + 1, n_asked - 1)
            for k in range(ahead, n_asked):
                pl.when(i + ahead == k)(tile_copies[k].start)
            for t in range(n):
                if t + 1 < n:
                    multiply(order[t + 1], (t + 1) % turns, i)
                else:
                    pl.when(i + 1 < n_asked)(functools.partial(arrive, later))
                    multiply(order[0], 0, later)
                consume(order[t], t % turns, i)
            return carry

        lax.fori_loop(begin, end, step, 0)
    if results:
        m = jnp.max(top[...], axis=0, keepdims=True)
        s = jnp.sum(total[...] * jnp.exp2((top[...] - m) * factor), axis=0, keepdims=True)
        p = jnp.sum(hit[...], axis=0, keepdims=True)
        seen = (count[...] + given[3][...] * (carried[1] / carried[2])) * (1.0 / n_asked)
        seen = jnp.concatenate([jnp.sum(seen, axis=0, keepdims=True)] * lanes, axis=1)
        for out, group in zip(answers, results):
            for h, i in enumerate(group):
                at, to = slice(i * TILE_Q, (i + 1) * TILE_Q), slice(h * TILE_Q, (h + 1) * TILE_Q)
                for row, value in enumerate((m[:, at], s[:, at], p[:, at], seen)):
                    out[row : row + 1, to] = value


def chunk(docs, tile_rows, firsts, asked, loops, given, carried, results, block0, slots, scale):
    deep = asked[0].shape[0]
    rows, feat = docs[0].shape
    width = len(asked) * TILE_Q
    n_tiles = len(docs) * rows // tile_rows
    state = [((8, width), jnp.float32)] * 3 + [((8, LANES), jnp.float32)]
    vmem, hbm = pl.BlockSpec(memory_space=pltpu.VMEM), pl.BlockSpec(memory_space=pltpu.HBM)
    turns = max(2 if len(o) % 2 == 0 else len(o) for _, _, o in loops)
    scratch = [
        pltpu.VMEM((n_tiles, tile_rows, feat), jnp.bfloat16),
        pltpu.VMEM((len(asked), deep, TILE_Q), jnp.bfloat16),
        pltpu.VMEM((turns, tile_rows, TILE_Q), jnp.float32),
        pltpu.SemaphoreType.DMA((len(docs),)),
        pltpu.SemaphoreType.DMA((len(asked),)),
    ]
    if results:
        out = [jax.ShapeDtypeStruct((4, len(g) * TILE_Q), jnp.float32) for g in results]
        scratch = [pltpu.VMEM(*s) for s in state] + scratch
    else:
        out = [jax.ShapeDtypeStruct(*s) for s in state]
    work = sum((e - b) * len(o) for b, e, o in loops) * tile_rows * TILE_Q
    plan = (len(docs), len(asked), loops, carried, results)
    return pl.pallas_call(
        functools.partial(kernel, plan, block0, slots, scale),
        out_shape=out,
        in_specs=[pl.BlockSpec(memory_space=pltpu.SMEM)]
        + [hbm] * (len(docs) + len(asked))
        + [vmem] * len(given),
        out_specs=[vmem] * len(out),
        scratch_shapes=scratch,
        cost_estimate=pl.CostEstimate(flops=2 * work * feat, bytes_accessed=2 * deep * width, transcendentals=work),
        compiler_params=pltpu.CompilerParams(vmem_limit_bytes=VMEM_LIMIT),
    )(firsts, *docs, *asked, *given)


def losses_of(queries, documents, counts, positives):
    slots, feat = documents.shape
    scale = feat ** (-0.5)
    slot = lax.broadcasted_iota(jnp.int32, documents.shape, 0)
    buffer = jnp.where(slot < counts[0], documents, jnp.bfloat16(jnp.nan))
    mine = list(prepared(queries, positives))
    asked = [[by_offset(tile, o) for o in NEIGHBOURS] for tile in mine]
    held = [(0, 0, 0)]
    for offsets in NEAR:
        pieces = [by_offset(buffer, o) for o in offsets]
        held = held + [a for o in offsets for a in moved(held, o)]
        buffer = jnp.concatenate([buffer] + pieces, axis=0)
    parts = [buffer] + [by_offset(buffer, o) for o in FAR]
    firsts = first_indices([held, sum([moved(held, o) for o in FAR], [])], slots)
    theirs = [to_partner(part) for part in parts]
    common = (slots, scale)
    rows = buffer.shape[0]
    near, far = [parts[0], theirs[0]], parts[1:] + theirs[1:]
    n, m, late = len(NEIGHBOURS), len(mine), 2 * len(held)
    early = mine + asked[0]
    state = chunk(near, rows, firsts, early, ((0, len(early), (0, 1)),), (), (), (), 0, *common)
    answers = chunk(
        far + near, 2 * rows, again(firsts, late), asked[0] + asked[1],
        ((0, n, (0, 1, 2)), (n, 2 * n, (0, 1, 2, 3))), state, (m, n, m + n), tuple((k, n + k) for k in range(n)), 0, *common
    )
    own = chunk(
        far, 2 * rows, firsts, mine, ((0, m, (0, 1, 2)),), state, (0, m, m + n),
        (tuple(range(m)),), late, *common
    )[0]
    seen = answers[0][3]
    back = [by_offset(a, [-v for v in o]) for a, o in zip(answers, NEIGHBOURS)]
    top = functools.reduce(jnp.maximum, [a[0] for a in back], own[0])
    total = sum(a[1] * jnp.exp((a[0] - top) * scale) for a in [own] + back)
    hit = sum(a[2] for a in [own] + back)
    seen = seen + sum(a[3] for a in back)
    return top * scale + jnp.log(total) - hit * scale - jnp.log(seen)


def again(firsts, late):
    return jnp.concatenate([firsts[late:], firsts[:late]])


def solution(mesh):
    finer = Mesh(mesh.devices.reshape(2, 4, 2, 2, 8), AXES)
    return jax.shard_map(
        losses_of,
        mesh=finer,
        in_specs=(P(AXES, None), P(AXES, None), P(AXES), P(AXES)),
        out_specs=P(AXES),
        check_vma=False,
    )
```
